32 devices in a mesh: prow: 4 (over y, x), pcol: 8 (over z, core).
Axes of the slice: x: 2, y: 2, z: 4, core: 2. Of those that a mesh axis runs over, the one named last changes fastest.
Arguments:
- inverse_factor: float32 [1024, 1024], P('pcol'), as said below
- diag_block: float32 [1024, 1024], P('pcol'), as said below
- panel_matrix: float32 [16, 4, 128, 1024], P(None, 'prow', 'pcol'), may hold values from -6 to 6
- panel_factor: float32 [16, 4, 128, 1024], P(None, 'prow', 'pcol'), may hold values from -0.1875 to 0.1875
- trailing: float32 [16, 4, 128, 8, 8, 128], P(None, 'prow', None, None, 'pcol'), may hold values from -6 to 6
Outputs:
- reduced_diag: float32 [1024, 1024], P('pcol')
- panel_result: float32 [16, 4, 128, 1024], P(None, 'prow', 'pcol')
- trailing_out: float32 [16, 4, 128, 8, 8, 128], P(None, 'prow', None, None, 'pcol')
The draws below stay inside these ranges and needn't reach their ends.
Inputs may be any that keep to these rules, and one draw needn't show every extreme that they name: `inverse_factor`: lower triangular, diagonal entries between 0.5 and 2. `diag_block`: symmetric.
All inputs are finite; a program needn't handle non-finite values.
Results may differ from the reference program's by a relative error of at most 0.0003.
Values sent between devices are 32-bit elements; how exact they have to be, the bound alone decides.
No kernel may reach another device: no remote copies, remote signals or barrier semaphores. Data moves between devices by JAX's collectives and lax.ppermute only.
A program may use at most 128 MiB of HBM per device.

```python
import jax
import jax.numpy as jnp
from jax import lax

NB = 1024
TILE = 128
MR = 16
M = 8192
MC = 8
N_PROW = 4
N_PCOL = 8


def draw_inverse_factor(key, part):
    first, second = jax.random.split(jax.random.fold_in(key, 11), 2)
    spread = jax.random.normal(first, (NB, NB), jnp.float32) * (0.6 / NB ** 0.5)
    diagonal = jnp.exp(jax.random.uniform(second, (NB,), jnp.float32, -0.69, 0.69))
    return jnp.tril(spread, -1) + jnp.diag(diagonal)


def draw_diag_block(key, part):
    first = jax.random.fold_in(key, 23)
    base = jax.random.normal(first, (NB, NB), jnp.float32)
    return (base + base.T) * 0.70710678


def block_levels(stream_key, extent, cuts, low, largest):
    loudness = 1.0
    for axis_at, parts in cuts:
        steps = jax.random.uniform(jax.random.fold_in(jax.random.fold_in(stream_key, 6), axis_at), (parts,), jnp.float32, low / len(cuts), largest / len(cuts))
        loudness = loudness * jnp.repeat(jnp.exp(steps), extent[axis_at] // parts).reshape((-1,) + (1,) * (len(extent) - 1 - axis_at))
    return loudness


def centred(stream_key, extent, scale, most, pieces=(), held_as=jnp.bfloat16):
    entries = scale * jax.random.normal(stream_key, extent, jnp.float32)
    if pieces:
        entries = entries * block_levels(stream_key, extent, pieces, -0.22, 0.18)
    return jnp.clip(entries, -most, most).astype(held_as)


def setup_inputs(seed: int = 0) -> dict:
    keys = jax.random.split(jax.random.key(seed), 6)
    return {
        "inverse_factor": draw_inverse_factor(jax.random.fold_in(keys[5], 71), 0),
        "diag_block": draw_diag_block(jax.random.fold_in(keys[5], 71), 0),
        "panel_matrix": centred(keys[2], (MR, N_PROW, TILE, NB), 1.0, 6.0, ((1, 4), (2, 8)), jnp.float32),
        "panel_factor": centred(keys[3], (MR, N_PROW, TILE, NB), NB ** -0.5, 0.1875, ((1, 4), (2, 8)), jnp.float32),
        "trailing": centred(keys[4], (MR, N_PROW, TILE, MC, N_PCOL, TILE), 1.0, 6.0, ((1, 4), (4, 8)), jnp.float32),
    }


def reference(inverse_factor, diag_block, panel_matrix, panel_factor, trailing):
    exact = lax.Precision.HIGHEST
    order = M
    inner = jnp.dot(diag_block, inverse_factor.T, precision=exact, preferred_element_type=jnp.float32)
    reduced = jnp.dot(inverse_factor, inner, precision=exact, preferred_element_type=jnp.float32)
    panel = panel_matrix.reshape(order, NB)
    factor = panel_factor.reshape(order, NB)
    solved = jnp.dot(panel, inverse_factor.T, precision=exact, preferred_element_type=jnp.float32)
    coupled = jnp.dot(factor, reduced, precision=exact, preferred_element_type=jnp.float32)
    shifted = solved - 0.5 * coupled
    result = shifted - 0.5 * coupled
    whole = trailing.reshape(order, order)
    col_tile = jnp.arange(order, dtype=jnp.int32) // TILE

    def one_row(index):
        start = (index * TILE).astype(jnp.int32)
        rows_a = lax.dynamic_slice_in_dim(whole, start, TILE, 0)
        rows_y = lax.dynamic_slice_in_dim(shifted, start, TILE, 0)
        rows_f = lax.dynamic_slice_in_dim(factor, start, TILE, 0)
        update = jnp.dot(rows_y, factor.T, precision=exact, preferred_element_type=jnp.float32)
        update = update + jnp.dot(rows_f, shifted.T, precision=exact, preferred_element_type=jnp.float32)
        return jnp.where(col_tile[None, :] <= index, rows_a - update, rows_a)

    blocks = lax.map(one_row, jnp.arange(order // TILE, dtype=jnp.int32))
    trailing_out = blocks.reshape(trailing.shape)
    return reduced, result.reshape(panel_matrix.shape), trailing_out
```

```python
import functools

import jax
import jax.numpy as jnp
from jax import lax
from jax.experimental import pallas as pl
from jax.experimental.pallas import tpu as pltpu
from jax.sharding import PartitionSpec as P


F32 = jnp.float32
BF16 = jnp.bfloat16
EXTRA = 8


def split(x):
    high = x.astype(BF16)
    return high, (x - high.astype(F32)).astype(BF16)


def dot(a, b):
    return jnp.dot(a, b, preferred_element_type=F32)


def dot3(a, b_high, b_low):
    high, low = split(a)
    return dot(high, b_high) + (dot(low, b_high) + dot(high, b_low))


def dot_nt(a, b):
    return lax.dot_general(a, b, (((1,), (1,)), ((), ())), preferred_element_type=F32)


def call(kernel, outs, ins, scalars, scratch=(), grid=None, in_specs=None, out_specs=None, alias=None, flops=0):
    whole = pl.BlockSpec(memory_space=pltpu.VMEM)
    spec = pltpu.PrefetchScalarGridSpec(
        num_scalar_prefetch=1,
        grid=grid or (1,),
        in_specs=in_specs or [whole] * len(ins),
        out_specs=out_specs or [whole] * len(outs),
        scratch_shapes=list(scratch),
    )
    moved = sum(a.size * a.dtype.itemsize for a in (*ins, *outs))
    return pl.pallas_call(
        kernel,
        out_shape=outs,
        grid_spec=spec,
        input_output_aliases=alias or {},
        cost_estimate=pl.CostEstimate(flops=flops, bytes_accessed=moved, transcendentals=0),
        compiler_params=pltpu.CompilerParams(vmem_limit_bytes=50 * 2**20),
    )(jnp.stack([jnp.asarray(s, jnp.int32) for s in scalars]), *ins)


def unpack_kernel(s, rows, cols, extra, inv_h, inv_l, tr_h, tr_l, a_h, a_l):
    step = pl.program_id(0)
    size, width = rows.shape
    row = step * size + lax.broadcasted_iota(jnp.int32, (size, width), 0)
    col = lax.broadcasted_iota(jnp.int32, (size, width), 1)
    mine = rows[...]
    inv_h[...], inv_l[...] = split(jnp.where(row >= col, mine, 0.0))
    flipped = cols[...].T
    tr_h[...], tr_l[...] = split(jnp.where(col >= row, flipped, 0.0))
    diag = jnp.broadcast_to(extra[0, 0:1, 0:size], (size, size))
    spread = jnp.concatenate([diag] * (width // size), axis=1)
    a = jnp.where(col > row, mine, jnp.where(col < row, flipped, spread))
    a_h[...], a_l[...] = split(a)


def unpack(packed, extra):
    width = packed.shape[0]
    size = width // extra.shape[0]
    out = jax.ShapeDtypeStruct((width, width), BF16)
    row = pl.BlockSpec((size, width), lambda i, s: (i, 0))
    return call(
        unpack_kernel,
        [out] * 6,
        (packed, packed, extra),
        (0,),
        grid=(width // size,),
        in_specs=[row, pl.BlockSpec((width, size), lambda i, s: (0, i)), pl.BlockSpec((1, *extra.shape[1:]), lambda i, s: (i, 0, 0))],
        out_specs=[row] * 6,
        flops=10**9,
    )


def place_kernel(s, ref, out, extra):
    size = out.shape[0]
    out[...] = ref[0, 0, 0, 0:size, :]
    extra[...] = ref[0, 0, 0, size : size + EXTRA, :][None]


def place(stacked, line, core, grid_row, size):
    _, rows, length, _, part = stacked.shape
    shard = lambda i, s: 2 * ((i // rows) % length ^ s[0]) + (i // (rows * length) ^ s[1])
    out = jax.ShapeDtypeStruct((2 * length * size, rows * part), F32)
    extra = jax.ShapeDtypeStruct((2 * length, EXTRA, rows * part), F32)
    return call(
        place_kernel,
        [out, extra],
        (stacked,),
        (line, core, grid_row),
        grid=(2 * length * rows,),
        in_specs=[pl.BlockSpec((1, 1, 1, size + EXTRA, part), lambda i, s: (i // (rows * length), i % rows, (i // rows) % length, 0, 0))],
        out_specs=[
            pl.BlockSpec((size, part), lambda i, s: (shard(i, s), i % rows ^ s[2])),
            pl.BlockSpec((1, EXTRA, part), lambda i, s: (shard(i, s), 0, i % rows ^ s[2])),
        ],
        flops=10**8,
    )


def pair_of(panel, factor, mats):
    inv_h, inv_l, tr_h, tr_l, a_h, a_l = mats
    g = dot3(factor, inv_h[...], inv_l[...])
    rest = panel - dot3(g, a_h[...], a_l[...])
    return g, rest, (tr_h[...], tr_l[...])


def own_kernel(s, panel, factor, inv, *refs):
    *mats, reduced, result = refs
    width = panel.shape[-1]
    _, rest, flipped = pair_of(panel[...].reshape(-1, width), factor[...].reshape(-1, width), mats)
    result[...] = dot3(rest, *flipped).reshape(result.shape)
    reduced[...] = dot3(dot3(inv[...], mats[4][...], mats[5][...]), *flipped)


def column_kernel(carried, s, kept, got, *refs):
    mats, (out_h, out_l) = refs[:6], refs[6 + carried :]
    tiles, depth, wide = kept.shape[1:]
    first = s[1] == 0
    a, b = kept[...].reshape(-1, wide), got[...].reshape(-1, wide)
    g, rest, flipped = pair_of(jnp.where(first, a, b), jnp.where(first, b, a), mats)
    h = dot3(rest, *flipped)
    for at, value in ((0, g), (wide, h)):
        for piece, out in zip(split(value), (out_h, out_l), strict=True):
            for k in range(2):
                for j in range(tiles):
                    from_row = (k * tiles + j) * depth
                    out[j, k * depth : (k + 1) * depth, at : at + wide] = piece[from_row : from_row + depth]


def column(kept, got, mats, buffers, position, core, tile):
    _, tiles, depth, width = kept.shape
    whole = lambda a: pl.BlockSpec(a.shape, lambda i, s: (0,) * a.ndim)
    block = pl.BlockSpec((tiles, 2 * depth, 2 * width), lambda i, s: (0, s[0], 0))
    out = jax.ShapeDtypeStruct((tiles, tile, 2 * width), BF16)
    ins = (kept, got, *mats, *buffers)
    fixed = len(ins) - len(buffers)
    return call(
        functools.partial(column_kernel, len(buffers)),
        [out, out],
        ins,
        (position, core),
        in_specs=[whole(a) for a in ins[:fixed]] + [pl.BlockSpec(memory_space=pl.ANY)] * len(buffers),
        out_specs=[block, block],
        alias={fixed + 1 + n: n for n in range(len(buffers))},
        flops=18 * kept.size * width,
    )


def trailing_kernel(count, rows, s, *refs):
    units = refs[: 4 * count]
    g_h, g_l, _, out, lhs_h, lhs_l, acc, buf, sem = refs[4 * count :]
    step = pl.program_id(0)
    wanted, core, lead = s[count], s[count + 1], s[count + 2]
    tiles, depth, wide = units[0].shape[1:]
    group = 4 * depth
    per = count * group
    lines = 2 * depth * tiles

    def at(slot):
        start = pl.multiple_of(s[slot] * lines, lines)
        return out.at[:, pl.ds(start, lines), :]

    @pl.when(step == 0)
    def _():
        for slot in range(count):
            pltpu.make_async_copy(at(slot), buf.at[slot], sem.at[slot]).start()
        for slot in range(count):
            for unit in range(4):
                ref = units[4 * slot + unit]
                q = wanted if unit < 2 else 1 - wanted
                k = core if unit % 2 == 0 else 1 - core
                offset = pl.multiple_of(slot * group + q * 2 * depth + k * depth, depth)
                for half in range(2):
                    for j in range(tiles):
                        high, low = split(ref[half, j])
                        lhs_h[j, pl.ds(offset, depth), half * wide : (half + 1) * wide] = high
                        lhs_l[j, pl.ds(offset, depth), half * wide : (half + 1) * wide] = low
        for slot in range(count):
            pltpu.make_async_copy(at(slot), buf.at[slot], sem.at[slot]).wait()

    part = 256
    tile = g_h.shape[1]

    def block(n):
        height = (tiles - 2 * n) * per

        def one(i, first):
            here = pl.ds(pl.multiple_of(i * part, part), part)
            x_h = lhs_h[2 * n :, :, here].reshape(height, part)
            x_l = lhs_l[2 * n :, :, here].reshape(height, part)
            r_h = g_h[:, :, here].reshape(2 * tile, part)
            r_l = g_l[:, :, here].reshape(2 * tile, part)
            value = dot_nt(x_h, r_h) + dot_nt(x_l, r_h) + dot_nt(x_h, r_l)
            acc[0:height] = value if first else acc[0:height] + value

        one(0, True)
        lax.fori_loop(1, 2 * wide // part, lambda i, c: (one(i, False), c)[1], 0)
        for j in range(2 * n, tiles):
            for slot in range(count):
                for q in range(2):
                    base = (j - 2 * n) * per + slot * group + q * 2 * depth
                    for which in range(2):
                        column_tile = 2 * n + which
                        if column_tile > j:
                            continue
                        value = acc[base : base + 2 * depth, which * tile : (which + 1) * tile]
                        if column_tile == j:
                            value = jnp.where(rows * q + lead >= 0, value, 0.0)
                        there = pl.ds(column_tile, 2 * depth, stride=tiles)
                        buf[slot, 2 * j + q, there, :] = buf[slot, 2 * j + q, there, :] - value

    for n in range(tiles // 2):
        pl.when(step == n)(functools.partial(block, n))

    @pl.when(step == tiles // 2 - 1)
    def _():
        for slot in range(count):
            pltpu.make_async_copy(buf.at[slot], at(slot), sem.at[slot]).start()
        for slot in range(count):
            pltpu.make_async_copy(buf.at[slot], at(slot), sem.at[slot]).wait()


def update(slots, positions, wanted, core, lead, rows, high, low, state):
    units = [u for slot in slots for u in slot]
    count = len(slots)
    tiles, depth, wide = units[0].shape[1:]
    tile = high.shape[1]
    whole = pl.BlockSpec(units[0].shape, lambda i, s: (0, 0, 0, 0))
    right = pl.BlockSpec((2, tile, 2 * wide), lambda i, s: (i, 0, 0))
    any_space = pl.BlockSpec(memory_space=pl.ANY)
    ins = (*units, high, low, state)
    per = count * 4 * depth
    lhs = pltpu.VMEM((tiles, per, 2 * wide), BF16)
    return call(
        functools.partial(trailing_kernel, count, rows),
        [jax.ShapeDtypeStruct(state.shape, F32)],
        ins,
        (*positions, wanted, core, lead),
        scratch=[
            lhs,
            lhs,
            pltpu.VMEM((tiles * per, 2 * tile), F32),
            pltpu.VMEM((count, 2 * tiles, 2 * depth * tiles, tile), F32),
            pltpu.SemaphoreType.DMA((count,)),
        ],
        grid=(tiles // 2,),
        in_specs=[whole] * len(units) + [right, right, any_space],
        out_specs=[any_space],
        alias={len(ins): 0},
        flops=6 * tiles * per * 2 * wide * tiles * tile,
    )[0]


def permute(a, axis, pairs):
    return lax.ppermute(a, axis, pairs)


def fast_body(inverse_factor, diag_block, panel_matrix, panel_factor, trailing):
    rows, cols = lax.axis_size("prow"), lax.axis_size("pcol")
    length = cols // 2
    p, g = lax.axis_index("pcol"), lax.axis_index("prow")
    line, core = p // 2, p % 2
    size, width = inverse_factor.shape
    tile_rows, _, depth, _ = panel_matrix.shape
    tiles, tile = trailing.shape[3], trailing.shape[2]
    sel = jnp.where
    low_side = line < length // 2
    end = (line == 0) | (line == length - 1)
    wanted = p // rows

    outer = [(a, a ^ 2) for a in range(cols)]
    inner = [(2 * l + k, 2 * o + k) for a in range(1, length - 1, 2) for k in range(2) for l, o in ((a, a + 1), (a + 1, a))]
    A = lambda a: permute(a, "pcol", outer)
    B = lambda a: permute(a, "pcol", inner)
    D = lambda a: permute(a, "pcol", [(b, b ^ 1) for b in range(cols)])
    Y = lambda a: permute(a, "prow", [(b, b ^ 2) for b in range(rows)])
    X = lambda a: permute(a, "prow", [(b, b ^ 1) for b in range(rows)])

    row = p * size + lax.broadcasted_iota(jnp.int32, (size, width), 0)
    col = lax.broadcasted_iota(jnp.int32, (size, width), 1)
    diag = jnp.sum(sel(row == col, diag_block, 0.0), axis=1)
    mixed = sel(row >= col, inverse_factor, diag_block)
    part = width // rows
    quarter = lax.dynamic_slice_in_dim(mixed, g * part, part, 1)
    head = jnp.pad(diag[None], ((0, EXTRA - 1), (0, part - size)))
    quarter = jnp.concatenate([quarter, head])
    gathered = jnp.stack([quarter] + [permute(quarter, "pcol", [(a, a ^ (2 * k)) for a in range(cols)]) for k in range(1, length)])

    both = jnp.stack([panel_matrix, panel_factor]).reshape(2, tiles, 2, depth, width)
    want = sel(low_side, both[:, :, 0], both[:, :, 1])
    other = sel(low_side, both[:, :, 1], both[:, :, 0])

    a1f = A(sel(end, other, want))
    b1f = B(other)
    a2f = A(sel(end, want, b1f))
    b2f = B(a1f)
    a3f = A(b2f)
    a1s = A(other)
    b1s = B(want)
    a2s = A(b1s)
    b2s = B(a2f)
    a3s = A(b2s)
    first = [want, sel(end, a1f, b1f), sel(end, a2f, b2f), sel(end, a3f, a2f)]
    second = [other, sel(end, a1s, b1s), sel(end, a2s, b2s), sel(end, a3s, a1f)]
    first_swapped = [D(a) for a in first]
    second_swapped = [D(a) for a in second]
    slots = list(zip(first, first_swapped, second, second_swapped, strict=True))
    positions = [sel(low_side, line + n, line - n + length) % length for n in range(length)]

    m_two = jnp.stack([gathered, Y(gathered)])
    m_four = jnp.stack([m_two, X(m_two)], axis=1)
    m_all = jnp.stack([m_four, D(m_four)])
    packed, extra = place(m_all.reshape(2, rows, length, size + EXTRA, part), line, core, g, size)
    mats = unpack(packed, extra)

    def spread(own, swapped):
        mine = sel(core == 0, jnp.stack([own[0], swapped[0]]), jnp.stack([swapped[1], own[1]]))
        held = sel(g // 2 == line % 2, mine, Y(mine))
        across = X(held)
        send_across = (g % 2 == 0) == (core == 0)
        return sel(send_across, held, across), D(sel(send_across, across, held))

    buffers = ()
    for n in range(length):
        kept, got = spread(first[n], first_swapped[n])
        buffers = column(kept, got, mats, buffers, positions[n], core, tile)

    reduced, result = call(
        own_kernel,
        [jax.ShapeDtypeStruct((size, width), F32), jax.ShapeDtypeStruct((tile_rows, depth, width), F32)],
        (panel_matrix.reshape(tile_rows, depth, width), panel_factor.reshape(tile_rows, depth, width), inverse_factor, *mats),
        (0,),
        flops=18 * panel_matrix.size * width + 12 * size * width * width,
    )
    state = trailing.reshape(tile_rows, tile * tiles, tile)
    for some in (slice(0, 2), slice(2, 4)):
        state = update(slots[some], positions[some], wanted, core, g - p, rows, *buffers, state)
    return reduced, result.reshape(panel_matrix.shape), state.reshape(trailing.shape)


def broadcast(array, axis, root):
    mine = lax.axis_index(axis) == root
    return lax.psum(jnp.where(mine, array, jnp.zeros_like(array)), axis)


def plain_body(inverse_factor, diag_block, panel_matrix, panel_factor, trailing):
    exact = lax.Precision.HIGHEST
    grid_rows = lax.axis_size("prow")
    grid_cols = lax.axis_size("pcol")
    column = lax.axis_index("pcol")
    grid_row = lax.axis_index("prow")
    local_rows = inverse_factor.shape[0]
    width = inverse_factor.shape[1]
    inverse_full = lax.all_gather(inverse_factor, "pcol", axis=0, tiled=True)
    diag_terms = jnp.dot(
        diag_block, inverse_full.T, precision=exact, preferred_element_type=jnp.float32
    )
    terms_full = lax.all_gather(diag_terms, "pcol", axis=0, tiled=True)
    reduced = jnp.dot(inverse_full, terms_full, precision=exact, preferred_element_type=jnp.float32)
    reduced_rows = lax.dynamic_slice_in_dim(reduced, column * local_rows, local_rows, 0)
    shape = panel_matrix.shape
    solved = jnp.dot(
        panel_matrix.reshape(-1, width),
        inverse_full.T,
        precision=exact,
        preferred_element_type=jnp.float32,
    )
    coupled = jnp.dot(
        panel_factor.reshape(-1, width),
        reduced,
        precision=exact,
        preferred_element_type=jnp.float32,
    )
    shifted = solved - 0.5 * coupled
    panel_result = (shifted - 0.5 * coupled).reshape(shape)
    rows_y, rows_l = (
        lax.all_gather(shifted.reshape(shape), "pcol", axis=2, tiled=True),
        lax.all_gather(panel_factor, "pcol", axis=2, tiled=True),
    )
    tile_rows = rows_y.shape[0]
    tile = rows_y.shape[2]
    col_tiles = trailing.shape[3]
    stride = grid_cols // grid_rows
    picked = column // grid_rows

    def select(rows):
        grouped = rows.reshape(col_tiles, stride, tile, width)
        return lax.dynamic_index_in_dim(grouped, picked, 1, keepdims=False)

    col_y, col_l = (
        broadcast(select(rows_y), "prow", column % grid_rows),
        broadcast(select(rows_l), "prow", column % grid_rows),
    )
    rows_y = rows_y.reshape(tile_rows, tile, width)
    rows_l = rows_l.reshape(tile_rows, tile, width)
    block = trailing.reshape(tile_rows, tile, col_tiles, tile)
    row_ids = jnp.arange(tile_rows, dtype=jnp.int32) * grid_rows + grid_row
    col_ids = jnp.arange(col_tiles, dtype=jnp.int32) * grid_cols + column
    lower = (row_ids[:, None] >= col_ids[None, :])[:, None, :, None]
    update = jnp.einsum(
        "isk,jtk->isjt", rows_y, col_l, precision=exact, preferred_element_type=jnp.float32
    )
    update = update + jnp.einsum(
        "isk,jtk->isjt", rows_l, col_y, precision=exact, preferred_element_type=jnp.float32
    )
    result = jnp.where(lower, block - update, block)
    return (reduced_rows, panel_result, result.reshape(trailing.shape))


def solution(mesh):
    rows, cols = mesh.shape["prow"], mesh.shape["pcol"]
    in_specs = (
        P("pcol", None),
        P("pcol", None),
        P(None, "prow", "pcol", None),
        P(None, "prow", "pcol", None),
        P(None, "prow", None, None, "pcol", None),
    )
    out_specs = (
        P("pcol", None),
        P(None, "prow", "pcol", None),
        P(None, "prow", None, None, "pcol", None),
    )
    fast = rows == 4 and cols == 2 * rows

    def body(*args):
        return (fast_body if fast else plain_body)(*args)

    return jax.shard_map(body, mesh=mesh, in_specs=in_specs, out_specs=out_specs, check_vma=False)
```
